128 devices in a mesh: rows: 64 (over x_lo, y, z, core), cols: 2 (over x_hi).
Axes of the slice: x: 4 (x_hi: 2, x_lo: 2; x = x_hi * 2 + x_lo), y: 4, z: 4, core: 2. Of those that a mesh axis runs over, the one named last changes fastest.
Arguments:
- design: bfloat16 [131072, 6144], P('rows', 'cols'), may hold values from -0.015625 to 0.015625
- targets: bfloat16 [131072, 128], P('rows'), may hold values from -6 to 6
- col_scale: float32 [6144], P('cols'), may hold values from 0.1 to 1
Outputs:
- solution: float32 [6144, 128], P('cols', 'rows')
- residual: float32 [131072, 128], P('rows')
The draws below stay inside these ranges and needn't reach their ends.
All inputs are finite; a program needn't handle non-finite values.
Results may differ from the reference program's by a relative error of at most 0.0065.
Values may be sent and summed in bfloat16 or wider, within the bound.
No kernel may reach another device: no remote copies, remote signals or barrier semaphores. Data moves between devices by JAX's collectives and lax.ppermute only.
A program may use at most 128 MiB of HBM per device.

```python
import math
import jax
import jax.numpy as jnp
from jax import lax

P_SIZE = 6144
FITS = 128
ITERS = 6
M = 131072


def levels(key, shape, cuts, low, high):
    def one(axis_at, shards_of):
        draws = jax.random.uniform(jax.random.fold_in(jax.random.fold_in(key, 6), axis_at), (shards_of,), jnp.float32, low / len(cuts), high / len(cuts))
        return jnp.repeat(jnp.exp(draws), shape[axis_at] // shards_of).reshape((-1,) + (1,) * (len(shape) - axis_at - 1))

    level = one(*cuts[0])
    for cut in cuts[1:]:
        level = level * one(*cut)
    return level


def gaussian(own_key, extent, width, bound, pieces=(), held_as=jnp.bfloat16):
    gain = levels(own_key, extent, pieces, -0.22, 0.18) if pieces else 1.0
    values = jax.random.normal(own_key, extent, jnp.float32) * width * gain
    return jnp.minimum(jnp.maximum(values, -bound), bound).astype(held_as)


def setup_inputs(seed: int = 0) -> dict:
    seeds = jax.random.split(jax.random.key(seed), 4)
    design = gaussian(seeds[0], (M, P_SIZE), M ** -0.5, 0.015625, ((0, 64), (1, 2)))
    targets = gaussian(seeds[1], (M, FITS), 1.0, 6.0, ((0, 64),))
    col_scale = jnp.clip(jnp.exp(math.log(1.0) - 2.3025851 * jax.random.uniform(seeds[2], (P_SIZE,), jnp.float32) ** levels(seeds[2], (P_SIZE,), ((0, 2),), -0.2, 0.2)), 0.1, 1.0)
    return dict(design=design, targets=targets, col_scale=col_scale)


def back_apply(design, scale, vectors):
    product = lax.dot_general(design, vectors, (((0,), (0,)), ((), ())), preferred_element_type=jnp.float32)
    return scale * product


def reference(design, targets, col_scale):
    scale = col_scale[:, None]
    gradient = back_apply(design, scale, targets)
    gamma = jnp.sum(gradient * gradient, axis=0)
    solution = jnp.zeros(gradient.shape, jnp.float32)
    residual = targets.astype(jnp.float32)
    direction = gradient
    for step in range(ITERS):
        scaled_dir = (scale * direction).astype(jnp.bfloat16)
        image = jnp.dot(design, scaled_dir, preferred_element_type=jnp.float32)
        delta = jnp.sum(image * image, axis=0)
        alpha = gamma / delta
        solution = solution + alpha * direction
        residual = residual - alpha * image
        if step + 1 < ITERS:
            gradient = back_apply(design, scale, residual.astype(jnp.bfloat16))
            gamma_new = jnp.sum(gradient * gradient, axis=0)
            direction = gradient + (gamma_new / gamma) * direction
            gamma = gamma_new
    return solution, residual
```

```python
import functools

import jax
import jax.numpy as jnp
from jax import lax
from jax.sharding import Mesh
from jax.sharding import PartitionSpec as P

ITERS = 6
CHIPS = ("rows_0", "rows_1", "rows_2")
CORE = "rows_3"
ROWS = ("rows_0", "rows_1", "rows_2", "rows_3")
COLS = "cols"
BF16 = jnp.bfloat16
F32 = jnp.float32


def swapped(array, axis):
    return lax.ppermute(array, axis, ((0, 1), (1, 0)))


def local_back(design, vectors):
    return lax.dot_general(
        design, vectors, (((0,), (0,)), ((), ())), preferred_element_type=F32
    )


def local_image(design, vectors):
    return jnp.dot(design, vectors, preferred_element_type=F32)


def sum_over_rows(partial, square):
    core = lax.axis_index(CORE)
    chips = lax.axis_size(CHIPS)
    width, fits = partial.shape
    halves = partial.astype(BF16).reshape(2, width // 2, fits)
    kept = lax.dynamic_index_in_dim(halves, core, 0, False)
    given = lax.dynamic_index_in_dim(halves, 1 - core, 0, False)
    both = kept.astype(F32) + swapped(given, CORE).astype(F32)
    pieces = both.astype(BF16).reshape(chips, -1, fits)
    arrived = lax.all_to_all(pieces, CHIPS, split_axis=0, concat_axis=0, tiled=True)
    share = arrived.astype(F32).sum(axis=0)
    own = lax.axis_index(CORE) * chips + lax.axis_index(CHIPS)
    rows = share.shape[0]
    scaled = share * lax.dynamic_slice_in_dim(square, own * rows, rows, 0)
    copies = jnp.broadcast_to(scaled.astype(BF16), (chips, rows, fits))
    half = lax.all_to_all(copies, CHIPS, split_axis=0, concat_axis=0, tiled=True)
    half = half.reshape(width // 2, fits)
    other = swapped(half, CORE)
    low = jnp.where(core == 0, half, other)
    high = jnp.where(core == 0, other, half)
    return jnp.concatenate([low, high], axis=0)


def sum_over_cols(array):
    return array.astype(F32) + swapped(array, COLS).astype(F32)


def per_device(design, targets, col_scale):
    scale = col_scale[:, None]
    square = scale * scale
    weight = 1.0 / square
    width = design.shape[1]
    residual = targets.astype(F32)

    start = sum_over_rows(local_back(design, targets), square)
    gradient = start.astype(F32)
    gamma = sum_over_cols(jnp.sum(gradient * gradient * weight, axis=0))
    direction = gradient
    fit = jnp.zeros_like(gradient)
    moved = local_image(design, start)
    partial = moved
    for step in range(ITERS):
        image = sum_over_cols(partial.astype(BF16))
        if step + 1 < ITERS:
            back = sum_over_rows(local_back(design, image.astype(BF16)), square)
            back_image = local_image(design, back)
            back = back.astype(F32)
            weighted = back * weight
            sums = jnp.stack(
                [
                    jnp.sum(direction * weighted, axis=0),
                    jnp.sum(gradient * weighted, axis=0),
                    jnp.sum(back * weighted, axis=0),
                ]
            )
            sums = sum_over_cols(sums)
            delta = sums[0]
        else:
            delta = jnp.sum(image * image, axis=0)
            copies = jnp.broadcast_to(delta, (lax.axis_size(ROWS), 1, *delta.shape))
            delta = lax.all_to_all(copies, ROWS, split_axis=0, concat_axis=0, tiled=True)
            delta = delta.sum(axis=(0, 1))
        alpha = gamma / delta
        fit = fit + alpha * direction
        residual = residual - alpha * image
        if step + 1 < ITERS:
            gamma_new = gamma - 2.0 * alpha * sums[1] + alpha * alpha * sums[2]
            ratio = gamma_new / gamma
            gradient = gradient - alpha * back
            direction = gradient + ratio * direction
            moved = moved - alpha * back_image
            partial = moved + ratio * partial
            gamma = gamma_new
    fits = targets.shape[1]
    count = fits // lax.axis_size(ROWS)
    part = lax.dynamic_slice_in_dim(fit, lax.axis_index(ROWS) * count, count, 1)
    return part / scale, residual


def solution(mesh):
    split = Mesh(
        mesh.devices.reshape(2, 4, 4, 2, mesh.shape["cols"]),
        ("rows_0", "rows_1", "rows_2", "rows_3", "cols"),
    )
    in_specs = (P(ROWS, "cols"), P(ROWS, None), P("cols"))
    out_specs = (P("cols", ROWS), P(ROWS, None))
    return jax.shard_map(
        per_device, mesh=split, in_specs=in_specs, out_specs=out_specs, check_vma=False
    )
```

```python
import jax
import jax.numpy as jnp
from jax import lax
from jax.experimental import pallas as pl
from jax.experimental.pallas import tpu as pltpu
from jax.sharding import Mesh
from jax.sharding import PartitionSpec as P

ITERS = 6
CHIPS = ("rows_0", "rows_1", "rows_2")
CORE = "rows_3"
ROWS = ("rows_0", "rows_1", "rows_2", "rows_3")
COLS = "cols"
BF16 = jnp.bfloat16
F32 = jnp.float32
EXTRA = 16
ROW_BLOCK = 256
COL_BLOCK = 768


def swapped(array, axis):
    return lax.ppermute(array, axis, ((0, 1), (1, 0)))


def settings():
    return pltpu.CompilerParams(
        dimension_semantics=("arbitrary",), vmem_limit_bytes=24 * 1024 * 1024
    )


def price(rows, cols, fits):
    return pl.CostEstimate(
        flops=2 * rows * cols * fits, bytes_accessed=2 * rows * cols, transcendentals=0
    )


def whole(shape):
    return pl.BlockSpec(shape, lambda i, *_: (0,) * len(shape))


def image_step(design, vector, chunk, moved=None, alpha=None):
    rows, width = design.shape[0] // 2, design.shape[1]
    fits = vector.shape[1]
    steps = rows // ROW_BLOCK
    block = pl.BlockSpec((ROW_BLOCK, fits), lambda i: (i, 0))

    def kernel(d, v, *rest):
        product = jnp.dot(d[...], v[...], preferred_element_type=F32)
        if moved is not None:
            u, a, out, short = rest
            product = u[...] - a[...] * product
        else:
            out, short = rest
        out[...] = product
        short[...] = product.astype(BF16)

    in_specs = [
        pl.BlockSpec((ROW_BLOCK, width), lambda i: (chunk * steps + i, 0)),
        whole((width, fits)),
    ]
    args = [design, vector]
    if moved is not None:
        in_specs += [block, whole((1, fits))]
        args += [moved, alpha]
    return pl.pallas_call(
        kernel,
        grid=(steps,),
        in_specs=in_specs,
        out_specs=[block, block],
        out_shape=[
            jax.ShapeDtypeStruct((rows, fits), F32),
            jax.ShapeDtypeStruct((rows, fits), BF16),
        ],
        compiler_params=settings(),
        cost_estimate=price(rows, width, fits),
    )(*args)


def start_back(side, design, vectors):
    rows, width = design.shape
    fits = vectors.shape[1]
    half, block = width // 2, COL_BLOCK // 2
    steps = half // block

    def kernel(s, d, v, out, turned):
        @pl.when(pl.program_id(0) == 0)
        def _():
            turned[...] = v[...].T

        out[...] = jnp.dot(turned[...], d[...], preferred_element_type=F32).T.astype(BF16)

    return pl.pallas_call(
        kernel,
        grid_spec=pltpu.PrefetchScalarGridSpec(
            num_scalar_prefetch=1,
            grid=(steps,),
            in_specs=[
                pl.BlockSpec((rows, block), lambda i, s: (0, s[0] * steps + i)),
                whole((rows, fits)),
            ],
            out_specs=pl.BlockSpec((block, fits), lambda i, s: (i, 0)),
            scratch_shapes=[pltpu.VMEM((fits, rows), BF16)],
        ),
        out_shape=jax.ShapeDtypeStruct((half, fits), BF16),
        compiler_params=settings(),
        cost_estimate=price(rows, half, fits),
    )(side, design, vectors)


def joined(own, other, prior, ratio):
    total = own[...].astype(F32) + other[...].astype(F32)
    if prior is not None:
        total = total + ratio[...] * prior[...]
    return total


def back_first(design, own, other, prior, ratio):
    rows, width = own.shape[0], design.shape[1]
    fits = own.shape[1]
    steps = width // COL_BLOCK
    follow = prior is not None

    def kernel(d, own_ref, other_ref, *rest):
        if follow:
            prior_ref, ratio_ref, out, image, norm, turned = rest
        else:
            prior_ref = ratio_ref = None
            out, image, norm, turned = rest

        @pl.when(pl.program_id(0) == 0)
        def _():
            total = joined(own_ref, other_ref, prior_ref, ratio_ref)
            image[...] = total
            norm[...] = jnp.sum(total * total, axis=0, keepdims=True)
            turned[...] = total.astype(BF16).T

        out[...] = jnp.dot(turned[...], d[...], preferred_element_type=F32).T

    piece = whole((rows, fits))
    in_specs = [pl.BlockSpec((rows, COL_BLOCK), lambda i: (0, i)), piece, piece]
    args = [design, own, other]
    if follow:
        in_specs += [piece, whole((1, fits))]
        args += [prior, ratio]
    return pl.pallas_call(
        kernel,
        grid=(steps,),
        in_specs=in_specs,
        out_specs=[
            pl.BlockSpec((COL_BLOCK, fits), lambda i: (i, 0)),
            piece,
            whole((1, fits)),
        ],
        out_shape=[
            jax.ShapeDtypeStruct((width, fits), F32),
            jax.ShapeDtypeStruct((rows, fits), F32),
            jax.ShapeDtypeStruct((1, fits), F32),
        ],
        scratch_shapes=[pltpu.VMEM((fits, rows), BF16)],
        compiler_params=settings(),
        cost_estimate=price(rows, width, fits),
    )(*args)


def back_given(side, design, own, other, prior, ratio, begun, norm_first):
    rows, width = own.shape[0], design.shape[1]
    fits = own.shape[1]
    half = width // 2
    steps = half // COL_BLOCK
    follow = prior is not None

    def kernel(s, d, own_ref, other_ref, begun_ref, norm_ref, *rest):
        if follow:
            prior_ref, ratio_ref, out, image, turned, norm = rest
        else:
            prior_ref = ratio_ref = None
            out, image, turned, norm = rest

        step = pl.program_id(0)

        @pl.when(step == 0)
        def _():
            total = joined(own_ref, other_ref, prior_ref, ratio_ref)
            image[...] = total
            turned[...] = total.astype(BF16).T
            norms = norm_ref[...] + jnp.sum(total * total, axis=0, keepdims=True)
            norm[...] = norms
            high = norms.astype(BF16).astype(F32)
            middle = (norms - high).astype(BF16).astype(F32)
            low = norms - high - middle
            row = lax.broadcasted_iota(jnp.int32, (EXTRA, fits), 0)
            below = jnp.where(row == 0, high, jnp.where(row == 1, middle, low))
            out[pl.ds(half, EXTRA), :] = jnp.where(row < 3, below, 0.0).astype(BF16)

        product = jnp.dot(turned[...], d[...], preferred_element_type=F32).T
        where = pl.multiple_of(step * COL_BLOCK, COL_BLOCK)
        out[pl.ds(where, COL_BLOCK), :] = (product + begun_ref[...]).astype(BF16)

    piece = whole((rows, fits))
    block = lambda i, s: (s[0] * steps + i, 0)
    in_specs = [
        pl.BlockSpec((rows, COL_BLOCK), lambda i, s: (1, s[0] * steps + i)),
        piece,
        piece,
        pl.BlockSpec((COL_BLOCK, fits), block),
        whole((1, fits)),
    ]
    args = [design, own, other, begun, norm_first]
    if follow:
        in_specs += [piece, whole((1, fits))]
        args += [prior, ratio]
    return pl.pallas_call(
        kernel,
        grid_spec=pltpu.PrefetchScalarGridSpec(
            num_scalar_prefetch=1,
            grid=(steps,),
            in_specs=in_specs,
            out_specs=[
                whole((half + EXTRA, fits)),
                piece,
                whole((fits, rows)),
                whole((1, fits)),
            ],
        ),
        out_shape=[
            jax.ShapeDtypeStruct((half + EXTRA, fits), BF16),
            jax.ShapeDtypeStruct((rows, fits), F32),
            jax.ShapeDtypeStruct((fits, rows), BF16),
            jax.ShapeDtypeStruct((1, fits), F32),
        ],
        compiler_params=settings(),
        cost_estimate=price(rows, half, fits),
    )(side, *args)


def back_kept(side, design, turned, begun):
    fits, rows = turned.shape
    half = design.shape[1] // 2
    steps = half // COL_BLOCK

    def kernel(s, d, t, begun_ref, out):
        product = jnp.dot(t[...], d[...], preferred_element_type=F32).T
        out[...] = product + begun_ref[...]

    block = lambda i, s: (s[0] * steps + i, 0)
    return pl.pallas_call(
        kernel,
        grid_spec=pltpu.PrefetchScalarGridSpec(
            num_scalar_prefetch=1,
            grid=(steps,),
            in_specs=[
                pl.BlockSpec((rows, COL_BLOCK), lambda i, s: (1, s[0] * steps + i)),
                whole((fits, rows)),
                pl.BlockSpec((COL_BLOCK, fits), block),
            ],
            out_specs=pl.BlockSpec((COL_BLOCK, fits), lambda i, s: (i, 0)),
        ),
        out_shape=jax.ShapeDtypeStruct((half, fits), F32),
        compiler_params=settings(),
        cost_estimate=price(rows, half, fits),
    )(side, design, turned, begun)


def exchanged(pieces):
    return lax.all_to_all(pieces, CHIPS, split_axis=0, concat_axis=0, tiled=True)


def whole_half(share, square):
    core = lax.axis_index(CORE)
    chips = lax.axis_size(CHIPS)
    rows, fits = share.shape
    scaled = (share * square).astype(BF16)
    half = exchanged(jnp.broadcast_to(scaled, (chips, rows, fits))).reshape(-1, fits)
    other = swapped(half, CORE)
    low = jnp.where(core == 0, half, other)
    high = jnp.where(core == 0, other, half)
    return jnp.concatenate([low, high], axis=0)


def per_device(design, targets, col_scale):
    core = lax.axis_index(CORE)
    chips = lax.axis_size(CHIPS)
    width, fits = design.shape[1], targets.shape[1]
    depth = targets.shape[0] // 2
    half = width // 2
    mine = core.astype(jnp.int32).reshape(1)
    theirs = 1 - mine
    rows = half // chips
    own = core * chips + lax.axis_index(CHIPS)
    square = lax.dynamic_slice_in_dim(col_scale, own * rows, rows, 0)[:, None]
    square = square * square
    weight = 1.0 / (col_scale * col_scale)[:, None]
    count = fits // lax.axis_size(ROWS)
    first = lax.axis_index(ROWS) * count
    picks = lax.broadcasted_iota(jnp.int32, (count, fits), 1)
    picks = picks == first + lax.broadcasted_iota(jnp.int32, (count, fits), 0)
    picks = picks.astype(BF16)

    def picked(vector):
        return lax.dot_general(
            picks, vector, (((1,), (1,)), ((), ())), preferred_element_type=F32
        )

    def picked_row(values):
        return lax.dynamic_slice_in_dim(values, first, count, 1).reshape(count, 1)

    def weighed(values):
        return jnp.sum(values * values * weight, axis=0, keepdims=True)

    given = start_back(theirs, design, targets)
    arrived = swapped(given, CORE)
    kept = start_back(mine, design, targets)
    both = (kept.astype(F32) + arrived.astype(F32)).astype(BF16)
    share = exchanged(both.reshape(chips, rows, fits)).astype(F32).sum(axis=0)
    back = whole_half(share, square)
    gradient = back.astype(F32)
    narrow = picked(back)
    narrow_dir = narrow
    narrow_fit = jnp.zeros_like(narrow)
    residual = [targets[:depth].astype(F32), targets[depth:].astype(F32)]
    alpha = ratio = gamma = None
    moved, image = [None, None], [None, None]
    for step in range(ITERS):
        moved_first, short_first = image_step(design, back, 0, moved[0], alpha)
        other_first = swapped(short_first, COLS)
        if step:
            gradient = gradient - alpha * back.astype(F32)
        part = weighed(gradient)
        part, later = lax.optimization_barrier((part, back))
        gamma_new = part + swapped(part, COLS)
        moved_second, short_second = image_step(design, later, 1, moved[1], alpha)
        other_second = swapped(short_second, COLS)
        moved = [moved_first, moved_second]
        if step:
            residual = [r - alpha * q for r, q in zip(residual, image)]
            narrow_alpha = picked_row(alpha)
            narrow_fit = narrow_fit + narrow_alpha * narrow_dir
            narrow = narrow - narrow_alpha * picked(back)
            ratio = gamma_new / gamma
            narrow_dir = narrow + picked_row(ratio) * narrow_dir
            (residual, narrow, narrow_fit, narrow_dir, gradient, other_second) = (
                lax.optimization_barrier(
                    (residual, narrow, narrow_fit, narrow_dir, gradient, other_second)
                )
            )
        gamma = gamma_new
        if step + 1 < ITERS:
            begun, image_first, norm = back_first(
                design, short_first, other_first, image[0], ratio
            )
            given, image_second, turned, norm = back_given(
                theirs, design, short_second, other_second, image[1], ratio, begun, norm
            )
            arrived = swapped(given, CORE)
            kept = back_kept(mine, design, turned, begun)
            image = [image_first, image_second]
            both = (kept + arrived[:half].astype(F32)).astype(BF16)
            norms = norm + jnp.sum(arrived[half:].astype(F32), axis=0, keepdims=True)
            high = lax.reduce_precision(norms, 8, 7)
            middle = lax.reduce_precision(norms - high, 8, 7)
            low = norms - high - middle
            below = jnp.concatenate([high, middle, low], axis=0).astype(BF16)
            below = jnp.pad(below, ((0, EXTRA - 3), (0, 0)))
            pieces = jnp.concatenate(
                [
                    both.reshape(chips, rows, fits),
                    jnp.broadcast_to(below, (chips, EXTRA, fits)),
                ],
                axis=1,
            )
            sums = exchanged(pieces).astype(F32).sum(axis=0)
            delta = jnp.sum(sums[rows:], axis=0, keepdims=True)
            alpha = gamma / delta
            back = whole_half(sums[:rows], square)
        else:
            pairs = zip((short_first, short_second), (other_first, other_second), image)
            image = [a.astype(F32) + b.astype(F32) + ratio * q for a, b, q in pairs]
            norm = sum(jnp.sum(q * q, axis=0) for q in image)
            copies = jnp.broadcast_to(norm, (lax.axis_size(ROWS), 1, fits))
            copies = lax.all_to_all(copies, ROWS, split_axis=0, concat_axis=0, tiled=True)
            delta = copies.sum(axis=0)
            alpha = gamma / delta
    residual = [r - alpha * q for r, q in zip(residual, image)]
    narrow_fit = narrow_fit + picked_row(alpha) * narrow_dir
    part = (narrow_fit / col_scale).T
    return part, jnp.concatenate(residual, axis=0)


def solution(mesh):
    split = Mesh(
        mesh.devices.reshape(2, 4, 4, 2, mesh.shape["cols"]),
        ("rows_0", "rows_1", "rows_2", "rows_3", "cols"),
    )
    in_specs = (P(ROWS, "cols"), P(ROWS, None), P("cols"))
    out_specs = (P("cols", ROWS), P(ROWS, None))
    return jax.shard_map(
        per_device, mesh=split, in_specs=in_specs, out_specs=out_specs, check_vma=False
    )
```

```python
import jax
import jax.numpy as jnp
from jax import lax
from jax.experimental import pallas as pl
from jax.experimental.pallas import tpu as pltpu
from jax.sharding import Mesh
from jax.sharding import PartitionSpec as P

ITERS = 6
CHIPS = ("rows_0", "rows_1", "rows_2")
CORE = "rows_3"
ROWS = ("rows_0", "rows_1", "rows_2", "rows_3")
COLS = "cols"
BF16 = jnp.bfloat16
F32 = jnp.float32
EXTRA = 16
ROW_BLOCK = 128
COL_BLOCK = 512
VMEM = 48 * 1024 * 1024


def swapped(array, axis):
    return lax.ppermute(array, axis, ((0, 1), (1, 0)))


def settings():
    return pltpu.CompilerParams(vmem_limit_bytes=VMEM)


def price(rows, cols, fits):
    return pl.CostEstimate(
        flops=2 * rows * cols * fits, bytes_accessed=2 * rows * cols, transcendentals=0
    )


ANYWHERE = pl.BlockSpec(memory_space=pltpu.HBM)
NEAR = pl.BlockSpec(memory_space=pltpu.VMEM)
SCALAR = pl.BlockSpec(memory_space=pltpu.SMEM)


def called(kernel, ins, specs, outs, held, steps, cost, extra=()):
    return pl.pallas_call(
        kernel,
        in_specs=specs,
        out_specs=[NEAR] * len(outs),
        out_shape=[jax.ShapeDtypeStruct(shape, dtype) for shape, dtype in outs],
        scratch_shapes=[
            pltpu.VMEM(held, BF16),
            pltpu.SemaphoreType.DMA((steps,)),
            *extra,
        ],
        compiler_params=settings(),
        cost_estimate=cost,
    )(*ins)


def started(fetch, steps):
    @pl.loop(0, steps)
    def _(i):
        fetch(i).start()


def image_step(design, vector, chunk, moved=None, alpha=None):
    rows, width = design.shape[0] // 2, design.shape[1]
    fits = vector.shape[1]
    steps = rows // ROW_BLOCK

    def kernel(d, v, *rest):
        if moved is not None:
            u, a, out, short, held, sems = rest
        else:
            out, short, held, sems = rest

        def fetch(i):
            return pltpu.make_async_copy(
                d.at[pl.ds(chunk * rows + i * ROW_BLOCK, ROW_BLOCK), :],
                held.at[i],
                sems.at[i],
            )

        started(fetch, steps)

        @pl.loop(0, steps)
        def _(i):
            fetch(i).wait()
            where = pl.ds(pl.multiple_of(i * ROW_BLOCK, ROW_BLOCK), ROW_BLOCK)
            product = jnp.dot(held[i], v[...], preferred_element_type=F32)
            if moved is not None:
                product = u[where, :] - a[...] * product
            out[where, :] = product
            short[where, :] = product.astype(BF16)

    args, specs = [design, vector], [ANYWHERE, NEAR]
    if moved is not None:
        args, specs = args + [moved, alpha], specs + [NEAR, NEAR]
    return called(
        kernel,
        args,
        specs,
        [((rows, fits), F32), ((rows, fits), BF16)],
        (steps, ROW_BLOCK, width),
        steps,
        price(rows, width, fits),
    )


def fetcher(d, held, sems, first_row, rows, first_col, block):
    def fetch(i):
        return pltpu.make_async_copy(
            d.at[
                pl.ds(first_row, rows),
                pl.ds(pl.multiple_of(first_col + i * block, block), block),
            ],
            held.at[i],
            sems.at[i],
        )

    return fetch


def start_back(side, design, vectors):
    rows, width = design.shape
    fits = vectors.shape[1]
    half, block = width // 2, COL_BLOCK // 2
    steps = half // block

    def kernel(s, d, v, out, held, sems, turned):
        fetch = fetcher(d, held, sems, 0, rows, s[0] * half, block)
        started(fetch, steps)
        turned[...] = v[...].T

        @pl.loop(0, steps)
        def _(i):
            fetch(i).wait()
            product = jnp.dot(turned[...], held[i], preferred_element_type=F32)
            out[pl.ds(pl.multiple_of(i * block, block), block), :] = product.T.astype(BF16)

    return called(
        kernel,
        [side, design, vectors],
        [SCALAR, ANYWHERE, NEAR],
        [((half, fits), BF16)],
        (steps, rows, block),
        steps,
        price(rows, half, fits),
        [pltpu.VMEM((fits, rows), BF16)],
    )[0]


def joined(own, other, prior, ratio):
    total = own[...].astype(F32) + other[...].astype(F32)
    if prior is not None:
        total = total + ratio[...] * prior[...]
    return total


def back_first(design, own, other, prior, ratio):
    rows, width = own.shape[0], design.shape[1]
    fits = own.shape[1]
    steps = width // COL_BLOCK
    follow = prior is not None

    def kernel(d, own_ref, other_ref, *rest):
        prior_ref = ratio_ref = None
        if follow:
            prior_ref, ratio_ref, *rest = rest
        out, image, norm, held, sems, turned = rest
        fetch = fetcher(d, held, sems, 0, rows, 0, COL_BLOCK)
        started(fetch, steps)
        total = joined(own_ref, other_ref, prior_ref, ratio_ref)
        image[...] = total
        norm[...] = jnp.sum(total * total, axis=0, keepdims=True)
        turned[...] = total.astype(BF16).T

        @pl.loop(0, steps)
        def _(i):
            fetch(i).wait()
            product = jnp.dot(turned[...], held[i], preferred_element_type=F32)
            out[pl.ds(pl.multiple_of(i * COL_BLOCK, COL_BLOCK), COL_BLOCK), :] = product.T

    args, specs = [design, own, other], [ANYWHERE, NEAR, NEAR]
    if follow:
        args, specs = args + [prior, ratio], specs + [NEAR, NEAR]
    return called(
        kernel,
        args,
        specs,
        [((width, fits), F32), ((rows, fits), F32), ((1, fits), F32)],
        (steps, rows, COL_BLOCK),
        steps,
        price(rows, width, fits),
        [pltpu.VMEM((fits, rows), BF16)],
    )


def back_given(side, design, own, other, prior, ratio, begun, norm_first):
    rows, width = own.shape[0], design.shape[1]
    fits = own.shape[1]
    half = width // 2
    steps = half // COL_BLOCK
    follow = prior is not None

    def kernel(s, d, own_ref, other_ref, begun_ref, norm_ref, *rest):
        prior_ref = ratio_ref = None
        if follow:
            prior_ref, ratio_ref, *rest = rest
        out, image, turned, norm, held, sems = rest
        fetch = fetcher(d, held, sems, rows, rows, s[0] * half, COL_BLOCK)
        started(fetch, steps)
        total = joined(own_ref, other_ref, prior_ref, ratio_ref)
        image[...] = total
        turned[...] = total.astype(BF16).T
        norms = norm_ref[...] + jnp.sum(total * total, axis=0, keepdims=True)
        norm[...] = norms
        high = norms.astype(BF16).astype(F32)
        middle = (norms - high).astype(BF16).astype(F32)
        low = norms - high - middle
        row = lax.broadcasted_iota(jnp.int32, (EXTRA, fits), 0)
        below = jnp.where(row == 0, high, jnp.where(row == 1, middle, low))
        out[pl.ds(half, EXTRA), :] = jnp.where(row < 3, below, 0.0).astype(BF16)

        @pl.loop(0, steps)
        def _(i):
            fetch(i).wait()
            where = pl.multiple_of(s[0] * half + i * COL_BLOCK, COL_BLOCK)
            product = jnp.dot(turned[...], held[i], preferred_element_type=F32).T
            product = product + begun_ref[pl.ds(where, COL_BLOCK), :]
            out[pl.ds(pl.multiple_of(i * COL_BLOCK, COL_BLOCK), COL_BLOCK), :] = product.astype(BF16)

    args = [side, design, own, other, begun, norm_first]
    specs = [SCALAR, ANYWHERE, NEAR, NEAR, NEAR, NEAR]
    if follow:
        args, specs = args + [prior, ratio], specs + [NEAR, NEAR]
    return called(
        kernel,
        args,
        specs,
        [
            ((half + EXTRA, fits), BF16),
            ((rows, fits), F32),
            ((fits, rows), BF16),
            ((1, fits), F32),
        ],
        (steps, rows, COL_BLOCK),
        steps,
        price(rows, half, fits),
    )


def back_kept(side, design, turned, begun):
    fits, rows = turned.shape
    half = design.shape[1] // 2
    steps = half // COL_BLOCK

    def kernel(s, d, t, begun_ref, out, held, sems):
        fetch = fetcher(d, held, sems, rows, rows, s[0] * half, COL_BLOCK)
        started(fetch, steps)

        @pl.loop(0, steps)
        def _(i):
            fetch(i).wait()
            where = pl.multiple_of(s[0] * half + i * COL_BLOCK, COL_BLOCK)
            product = jnp.dot(t[...], held[i], preferred_element_type=F32).T
            product = product + begun_ref[pl.ds(where, COL_BLOCK), :]
            out[pl.ds(pl.multiple_of(i * COL_BLOCK, COL_BLOCK), COL_BLOCK), :] = product

    return called(
        kernel,
        [side, design, turned, begun],
        [SCALAR, ANYWHERE, NEAR, NEAR],
        [((half, fits), F32)],
        (steps, rows, COL_BLOCK),
        steps,
        price(rows, half, fits),
    )[0]


def exchanged(pieces):
    return lax.all_to_all(pieces, CHIPS, split_axis=0, concat_axis=0, tiled=True)


def whole_half(share, square):
    core = lax.axis_index(CORE)
    chips = lax.axis_size(CHIPS)
    rows, fits = share.shape
    scaled = (share * square).astype(BF16)
    half = exchanged(jnp.broadcast_to(scaled, (chips, rows, fits))).reshape(-1, fits)
    other = swapped(half, CORE)
    low = jnp.where(core == 0, half, other)
    high = jnp.where(core == 0, other, half)
    return jnp.concatenate([low, high], axis=0)


def per_device(design, targets, col_scale):
    core = lax.axis_index(CORE)
    chips = lax.axis_size(CHIPS)
    width, fits = design.shape[1], targets.shape[1]
    depth = targets.shape[0] // 2
    half = width // 2
    mine = core.astype(jnp.int32).reshape(1)
    theirs = 1 - mine
    rows = half // chips
    own = core * chips + lax.axis_index(CHIPS)
    square = lax.dynamic_slice_in_dim(col_scale, own * rows, rows, 0)[:, None]
    square = square * square
    weight = 1.0 / (col_scale * col_scale)[:, None]
    count = fits // lax.axis_size(ROWS)
    first = lax.axis_index(ROWS) * count
    picks = lax.broadcasted_iota(jnp.int32, (count, fits), 1)
    picks = picks == first + lax.broadcasted_iota(jnp.int32, (count, fits), 0)
    picks = picks.astype(BF16)

    def picked(vector):
        return lax.dot_general(
            picks, vector, (((1,), (1,)), ((), ())), preferred_element_type=F32
        )

    def picked_row(values):
        return lax.dynamic_slice_in_dim(values, first, count, 1).reshape(count, 1)

    def weighed(values):
        return jnp.sum(values * values * weight, axis=0, keepdims=True)

    given = start_back(theirs, design, targets)
    arrived = swapped(given, CORE)
    kept = start_back(mine, design, targets)
    both = (kept.astype(F32) + arrived.astype(F32)).astype(BF16)
    share = exchanged(both.reshape(chips, rows, fits)).astype(F32).sum(axis=0)
    back = whole_half(share, square)
    gradient = back.astype(F32)
    narrow = picked(back)
    narrow_dir = narrow
    narrow_fit = jnp.zeros_like(narrow)
    residual = [targets[:depth].astype(F32), targets[depth:].astype(F32)]
    alpha = ratio = gamma = None
    moved, image = [None, None], [None, None]
    for step in range(ITERS):
        moved_first, short_first = image_step(design, back, 0, moved[0], alpha)
        other_first = swapped(short_first, COLS)
        short_first, back = lax.optimization_barrier((short_first, back))
        if step:
            gradient = gradient - alpha * back.astype(F32)
        part = weighed(gradient)
        part, back, gradient = lax.optimization_barrier((part, back, gradient))
        gamma_new = part + swapped(part, COLS)
        moved_second, short_second = image_step(design, back, 1, moved[1], alpha)
        other_second = swapped(short_second, COLS)
        moved = [moved_first, moved_second]
        if step:
            image, back, short_second = lax.optimization_barrier(
                (image, back, short_second)
            )
            residual = [r - alpha * q for r, q in zip(residual, image)]
            narrow_alpha = picked_row(alpha)
            narrow_fit = narrow_fit + narrow_alpha * narrow_dir
            narrow = narrow - narrow_alpha * picked(back)
            ratio = gamma_new / gamma
            narrow_dir = narrow + picked_row(ratio) * narrow_dir
            (residual, narrow, narrow_fit, narrow_dir, gradient, other_second) = (
                lax.optimization_barrier(
                    (residual, narrow, narrow_fit, narrow_dir, gradient, other_second)
                )
            )
        gamma = gamma_new
        if step + 1 < ITERS:
            begun, image_first, norm = back_first(design, short_first, other_first, image[0], ratio)
            given, image_second, turned, norm = back_given(
                theirs, design, short_second, other_second, image[1], ratio, begun, norm
            )
            arrived = swapped(given, CORE)
            kept = back_kept(mine, design, turned, begun)
            image = [image_first, image_second]
            both = (kept + arrived[:half].astype(F32)).astype(BF16)
            norms = norm + jnp.sum(arrived[half:].astype(F32), axis=0, keepdims=True)
            high = lax.reduce_precision(norms, 8, 7)
            middle = lax.reduce_precision(norms - high, 8, 7)
            low = norms - high - middle
            below = jnp.concatenate([high, middle, low], axis=0).astype(BF16)
            below = jnp.pad(below, ((0, EXTRA - 3), (0, 0)))
            pieces = jnp.concatenate(
                [both.reshape(chips, rows, fits), jnp.broadcast_to(below, (chips, EXTRA, fits))],
                axis=1,
            )
            sums = exchanged(pieces).astype(F32).sum(axis=0)
            delta = jnp.sum(sums[rows:], axis=0, keepdims=True)
            alpha = gamma / delta
            back = whole_half(sums[:rows], square)
        else:
            pairs = zip((short_first, short_second), (other_first, other_second), image)
            image = [a.astype(F32) + b.astype(F32) + ratio * q for a, b, q in pairs]
            norm = sum(jnp.sum(q * q, axis=0) for q in image)
            copies = jnp.broadcast_to(norm, (lax.axis_size(ROWS), 1, fits))
            copies = lax.all_to_all(copies, ROWS, split_axis=0, concat_axis=0, tiled=True)
            delta = copies.sum(axis=0)
            alpha = gamma / delta
    residual = [r - alpha * q for r, q in zip(residual, image)]
    narrow_fit = narrow_fit + picked_row(alpha) * narrow_dir
    part = (narrow_fit / col_scale).T
    return part, jnp.concatenate(residual, axis=0)


def solution(mesh):
    split = Mesh(
        mesh.devices.reshape(2, 4, 4, 2, mesh.shape["cols"]),
        ("rows_0", "rows_1", "rows_2", "rows_3", "cols"),
    )
    in_specs = (P(ROWS, "cols"), P(ROWS, None), P("cols"))
    out_specs = (P("cols", ROWS), P(ROWS, None))
    return jax.shard_map(
        per_device, mesh=split, in_specs=in_specs, out_specs=out_specs, check_vma=False
    )
```

```python
import jax
import jax.numpy as jnp
from jax import lax
from jax.experimental import pallas as pl
from jax.experimental.pallas import tpu as pltpu
from jax.sharding import Mesh
from jax.sharding import PartitionSpec as P

ITERS = 6
CHIPS = ("rows_0", "rows_1", "rows_2")
CORE = "rows_3"
ROWS = ("rows_0", "rows_1", "rows_2", "rows_3")
COLS = "cols"
BF16 = jnp.bfloat16
F32 = jnp.float32
EXTRA = 8
ROW_BLOCK = 128
COL_BLOCK = 512
START_BLOCK = 256
FAR_VMEM = 43 * 1024 * 1024
NEAR_VMEM = 8 * 1024 * 1024


def swapped(array, axis):
    return lax.ppermute(array, axis, ((0, 1), (1, 0)))


def settings(near):
    return pltpu.CompilerParams(vmem_limit_bytes=NEAR_VMEM if near else FAR_VMEM)


def price(rows, cols, fits):
    return pl.CostEstimate(
        flops=2 * rows * cols * fits, bytes_accessed=2 * rows * cols, transcendentals=0
    )


ANYWHERE = pl.BlockSpec(memory_space=pltpu.HBM)
NEAR = pl.BlockSpec(memory_space=pltpu.VMEM)
SCALAR = pl.BlockSpec(memory_space=pltpu.SMEM)


def called(kernel, ins, specs, outs, cost, scratch=(), near=True):
    return pl.pallas_call(
        kernel,
        in_specs=specs,
        out_specs=[NEAR] * len(outs),
        out_shape=[jax.ShapeDtypeStruct(shape, dtype) for shape, dtype in outs],
        scratch_shapes=list(scratch),
        compiler_params=settings(near),
        cost_estimate=cost,
    )(*ins)


def streamed(fetch, steps, work):
    @pl.loop(0, steps)
    def _(i):
        fetch(i).start()

    def ready(i):
        fetch(i).wait()
        work(i)

    pl.loop(0, steps)(ready)


def aligned(start, size):
    return pl.ds(pl.multiple_of(start, size), size)


def image_step(design, vector, chunk, moved=None, alpha=None):
    rows, width = design.shape[0] // 2, design.shape[1]
    fits = vector.shape[1]
    steps = rows // ROW_BLOCK

    def kernel(d, v, *rest):
        if moved is not None:
            u, a, out, short, close, sems = rest
        else:
            out, short, close, sems = rest

        def fetch(i):
            where = aligned(i * ROW_BLOCK, ROW_BLOCK)
            source = aligned(chunk * rows + i * ROW_BLOCK, ROW_BLOCK)
            return pltpu.make_async_copy(d.at[source, :], close.at[where, :], sems.at[i])

        def work(i):
            where = aligned(i * ROW_BLOCK, ROW_BLOCK)
            product = jnp.dot(close[where, :], v[...], preferred_element_type=F32)
            if moved is not None:
                product = u[where, :] - a[...] * product
            out[where, :] = product
            short[where, :] = product.astype(BF16)

        streamed(fetch, steps, work)

    args, specs = [design, vector], [ANYWHERE, NEAR]
    if moved is not None:
        args, specs = args + [moved, alpha], specs + [NEAR, NEAR]
    return called(
        kernel,
        args,
        specs,
        [((rows, fits), F32), ((rows, fits), BF16), ((rows, width), BF16)],
        price(rows, width, fits),
        [pltpu.SemaphoreType.DMA((steps,))],
        False,
    )


def start_back(side, design, vectors):
    rows, width = design.shape
    fits = vectors.shape[1]
    half, block = width // 2, START_BLOCK
    steps = half // block

    def kernel(s, d, v, out, turned, held, sems):
        def fetch(i):
            return pltpu.make_async_copy(
                d.at[:, aligned(s[0] * half + i * block, block)], held.at[i], sems.at[i]
            )

        turned[...] = v[...].T

        def work(i):
            product = jnp.dot(turned[...], held[i], preferred_element_type=F32)
            out[aligned(i * block, block), :] = product.T.astype(BF16)

        streamed(fetch, steps, work)

    return called(
        kernel,
        [side, design, vectors],
        [SCALAR, ANYWHERE, NEAR],
        [((half, fits), BF16)],
        price(rows, half, fits),
        [
            pltpu.VMEM((fits, rows), BF16),
            pltpu.VMEM((steps, rows, block), BF16),
            pltpu.SemaphoreType.DMA((steps,)),
        ],
        False,
    )[0]


def joined(own, other, prior, ratio):
    total = own[...].astype(F32) + other[...].astype(F32)
    if prior is not None:
        total = total + ratio[...] * prior[...]
    return total


def back_first(design, own, other, prior, ratio):
    rows, width = own.shape[0], design.shape[1]
    fits = own.shape[1]
    follow = prior is not None

    def kernel(d, own_ref, other_ref, *rest):
        prior_ref = ratio_ref = None
        if follow:
            prior_ref, ratio_ref, *rest = rest
        out, image, norm, turned = rest
        total = joined(own_ref, other_ref, prior_ref, ratio_ref)
        image[...] = total
        norm[...] = jnp.sum(total * total, axis=0, keepdims=True)
        turned[...] = total.astype(BF16).T

        @pl.loop(0, width // COL_BLOCK)
        def _(i):
            where = aligned(i * COL_BLOCK, COL_BLOCK)
            block = d[:, where]
            product = jnp.dot(turned[...], block, preferred_element_type=F32)
            out[where, :] = product.T

    args, specs = [design, own, other], [NEAR, NEAR, NEAR]
    if follow:
        args, specs = args + [prior, ratio], specs + [NEAR, NEAR]
    return called(
        kernel,
        args,
        specs,
        [((width, fits), F32), ((rows, fits), F32), ((1, fits), F32)],
        price(rows, width, fits),
        [pltpu.VMEM((fits, rows), BF16)],
    )


def back_given(side, design, own, other, prior, ratio, begun, norm_first):
    rows, width = own.shape[0], design.shape[1]
    fits = own.shape[1]
    half = width // 2
    follow = prior is not None

    def kernel(s, d, own_ref, other_ref, begun_ref, norm_ref, *rest):
        prior_ref = ratio_ref = None
        if follow:
            prior_ref, ratio_ref, *rest = rest
        out, image, turned, norm = rest
        total = joined(own_ref, other_ref, prior_ref, ratio_ref)
        image[...] = total
        turned[...] = total.astype(BF16).T
        norms = norm_ref[...] + jnp.sum(total * total, axis=0, keepdims=True)
        norm[...] = norms
        high = norms.astype(BF16).astype(F32)
        middle = (norms - high).astype(BF16).astype(F32)
        low = norms - high - middle
        row = lax.broadcasted_iota(jnp.int32, (EXTRA, fits), 0)
        below = jnp.where(row == 0, high, jnp.where(row == 1, middle, low))
        out[pl.ds(half, EXTRA), :] = jnp.where(row < 3, below, 0.0).astype(BF16)

        @pl.loop(0, half // COL_BLOCK)
        def _(i):
            where = aligned(s[0] * half + i * COL_BLOCK, COL_BLOCK)
            block = d[:, where]
            product = jnp.dot(turned[...], block, preferred_element_type=F32).T
            product = product + begun_ref[where, :]
            out[aligned(i * COL_BLOCK, COL_BLOCK), :] = product.astype(BF16)

    args = [side, design, own, other, begun, norm_first]
    specs = [SCALAR, NEAR, NEAR, NEAR, NEAR, NEAR]
    if follow:
        args, specs = args + [prior, ratio], specs + [NEAR, NEAR]
    return called(
        kernel,
        args,
        specs,
        [
            ((half + EXTRA, fits), BF16),
            ((rows, fits), F32),
            ((fits, rows), BF16),
            ((1, fits), F32),
        ],
        price(rows, half, fits),
    )


def back_kept(side, design, turned, begun):
    fits, rows = turned.shape
    half = design.shape[1] // 2

    def kernel(s, d, t, begun_ref, out):
        @pl.loop(0, half // COL_BLOCK)
        def _(i):
            where = aligned(s[0] * half + i * COL_BLOCK, COL_BLOCK)
            block = d[:, where]
            product = jnp.dot(t[...], block, preferred_element_type=F32).T
            out[aligned(i * COL_BLOCK, COL_BLOCK), :] = product + begun_ref[where, :]

    return called(
        kernel,
        [side, design, turned, begun],
        [SCALAR, NEAR, NEAR, NEAR],
        [((half, fits), F32)],
        price(rows, half, fits),
    )[0]


def exchanged(pieces):
    return lax.all_to_all(pieces, CHIPS, split_axis=0, concat_axis=0, tiled=True)


def whole_half(share, square):
    core = lax.axis_index(CORE)
    chips = lax.axis_size(CHIPS)
    rows, fits = share.shape
    scaled = (share * square).astype(BF16)
    half = exchanged(jnp.broadcast_to(scaled, (chips, rows, fits))).reshape(-1, fits)
    other = swapped(half, CORE)
    low = jnp.where(core == 0, half, other)
    high = jnp.where(core == 0, other, half)
    return jnp.concatenate([low, high], axis=0)


def per_device(design, targets, col_scale):
    core = lax.axis_index(CORE)
    chips = lax.axis_size(CHIPS)
    width, fits = design.shape[1], targets.shape[1]
    depth = targets.shape[0] // 2
    half = width // 2
    mine = core.astype(jnp.int32).reshape(1)
    theirs = 1 - mine
    rows = half // chips
    own = core * chips + lax.axis_index(CHIPS)
    square = lax.dynamic_slice_in_dim(col_scale, own * rows, rows, 0)[:, None]
    square = square * square
    weight = 1.0 / (col_scale * col_scale)[:, None]
    count = fits // lax.axis_size(ROWS)
    first = lax.axis_index(ROWS) * count
    picks = lax.broadcasted_iota(jnp.int32, (count, fits), 1)
    picks = picks == first + lax.broadcasted_iota(jnp.int32, (count, fits), 0)
    picks = picks.astype(BF16)

    def picked(vector):
        return lax.dot_general(
            picks, vector, (((1,), (1,)), ((), ())), preferred_element_type=F32
        )

    def picked_row(values):
        return lax.dynamic_slice_in_dim(values, first, count, 1).reshape(count, 1)

    def weighed(values):
        return jnp.sum(values * values * weight, axis=0, keepdims=True)

    given = start_back(theirs, design, targets)
    arrived = swapped(given, CORE)
    kept = start_back(mine, design, targets)
    both = (kept.astype(F32) + arrived.astype(F32)).astype(BF16)
    both, square, weight = lax.optimization_barrier((both, square, weight))
    share = exchanged(both.reshape(chips, rows, fits)).astype(F32).sum(axis=0)
    back = whole_half(share, square)
    gradient = back.astype(F32)
    narrow = picked(back)
    narrow_dir = narrow
    narrow_fit = jnp.zeros_like(narrow)
    residual = [targets[:depth].astype(F32), targets[depth:].astype(F32)]
    alpha = ratio = gamma = None
    moved, image = [None, None], [None, None]
    for step in range(ITERS):
        moved_first, short_first, rows_first = image_step(
            design, back, 0, moved[0], alpha
        )
        other_first = swapped(short_first, COLS)
        short_first, back = lax.optimization_barrier((short_first, back))
        if step:
            gradient = gradient - alpha * back.astype(F32)
        part = weighed(gradient)
        part, back, gradient = lax.optimization_barrier((part, back, gradient))
        gamma_new = part + swapped(part, COLS)
        moved_second, short_second, rows_second = image_step(design, back, 1, moved[1], alpha)
        other_second = swapped(short_second, COLS)
        moved = [moved_first, moved_second]
        if step:
            image, back, short_second = lax.optimization_barrier(
                (image, back, short_second)
            )
            residual = [r - alpha * q for r, q in zip(residual, image)]
            narrow_alpha = picked_row(alpha)
            narrow_fit = narrow_fit + narrow_alpha * narrow_dir
            narrow = narrow - narrow_alpha * picked(back)
            ratio = gamma_new / gamma
            narrow_dir = narrow + picked_row(ratio) * narrow_dir
            (residual, narrow, narrow_fit, narrow_dir, gradient, other_second) = (
                lax.optimization_barrier(
                    (residual, narrow, narrow_fit, narrow_dir, gradient, other_second)
                )
            )
        gamma = gamma_new
        if step + 1 < ITERS:
            begun, image_first, norm = back_first(
                rows_first, short_first, other_first, image[0], ratio
            )
            given, image_second, turned, norm = back_given(
                theirs, rows_second, short_second, other_second, image[1], ratio, begun, norm
            )
            arrived = swapped(given, CORE)
            kept = back_kept(mine, rows_second, turned, begun)
            image = [image_first, image_second]
            both = (kept + arrived[:half].astype(F32)).astype(BF16)
            norms = norm + jnp.sum(arrived[half:].astype(F32), axis=0, keepdims=True)
            high = lax.reduce_precision(norms, 8, 7)
            middle = lax.reduce_precision(norms - high, 8, 7)
            low = norms - high - middle
            below = jnp.concatenate([high, middle, low], axis=0).astype(BF16)
            below = jnp.pad(below, ((0, EXTRA - 3), (0, 0)))
            pieces = jnp.concatenate(
                [both.reshape(chips, rows, fits), jnp.broadcast_to(below, (chips, EXTRA, fits))],
                axis=1,
            )
            sums = exchanged(pieces).astype(F32).sum(axis=0)
            delta = jnp.sum(sums[rows:], axis=0, keepdims=True)
            alpha = gamma / delta
            back = whole_half(sums[:rows], square)
        else:
            pairs = zip((short_first, short_second), (other_first, other_second), image)
            image = [a.astype(F32) + b.astype(F32) + ratio * q for a, b, q in pairs]
            norm = sum(jnp.sum(q * q, axis=0) for q in image)
            copies = jnp.broadcast_to(norm, (lax.axis_size(ROWS), 1, fits))
            copies = lax.all_to_all(copies, ROWS, split_axis=0, concat_axis=0, tiled=True)
            delta = copies.sum(axis=0)
            alpha = gamma / delta
    residual = [r - alpha * q for r, q in zip(residual, image)]
    narrow_fit = narrow_fit + picked_row(alpha) * narrow_dir
    part = (narrow_fit / col_scale).T
    return part, jnp.concatenate(residual, axis=0)


def solution(mesh):
    split = Mesh(
        mesh.devices.reshape(2, 4, 4, 2, mesh.shape["cols"]),
        ("rows_0", "rows_1", "rows_2", "rows_3", "cols"),
    )
    in_specs = (P(ROWS, "cols"), P(ROWS, None), P("cols"))
    out_specs = (P("cols", ROWS), P(ROWS, None))
    return jax.shard_map(
        per_device, mesh=split, in_specs=in_specs, out_specs=out_specs, check_vma=False
    )
```

```python
import jax
import jax.numpy as jnp
from jax import lax
from jax.experimental import pallas as pl
from jax.experimental.pallas import tpu as pltpu
from jax.sharding import Mesh
from jax.sharding import PartitionSpec as P

ITERS = 6
CHIPS = ("rows_0", "rows_1", "rows_2")
CORE = "rows_3"
ROWS = ("rows_0", "rows_1", "rows_2", "rows_3")
COLS = "cols"
BF16 = jnp.bfloat16
F32 = jnp.float32
EXTRA = 8
ROW_BLOCK = 128
COL_BLOCK = 512
START_BLOCK = 256
FAR_VMEM = 42 * 1024 * 1024
NEAR_VMEM = 8 * 1024 * 1024


def swapped(array, axis):
    return lax.ppermute(array, axis, ((0, 1), (1, 0)))


def settings(near):
    return pltpu.CompilerParams(vmem_limit_bytes=NEAR_VMEM if near else FAR_VMEM)


def price(rows, cols, fits):
    return pl.CostEstimate(
        flops=2 * rows * cols * fits, bytes_accessed=2 * rows * cols, transcendentals=0
    )


ANYWHERE = pl.BlockSpec(memory_space=pltpu.HBM)
NEAR = pl.BlockSpec(memory_space=pltpu.VMEM)
SCALAR = pl.BlockSpec(memory_space=pltpu.SMEM)


def called(kernel, ins, specs, outs, cost, scratch=(), near=True):
    return pl.pallas_call(
        kernel,
        in_specs=specs,
        out_specs=[NEAR] * len(outs),
        out_shape=[jax.ShapeDtypeStruct(shape, dtype) for shape, dtype in outs],
        scratch_shapes=list(scratch),
        compiler_params=settings(near),
        cost_estimate=cost,
    )(*ins)


def streamed(fetch, steps, work):
    @pl.loop(0, steps)
    def _(i):
        fetch(i).start()

    def ready(i):
        fetch(i).wait()
        work(i)

    pl.loop(0, steps)(ready)


def aligned(start, size):
    return pl.ds(pl.multiple_of(start, size), size)


def image_step(design, vector, begin, rows, keep, moved=None, alpha=None):
    width, fits = design.shape[1], vector.shape[1]
    steps = rows // ROW_BLOCK

    def kernel(d, v, *rest):
        if moved is not None:
            u, a, out, short, close, sems = rest
        else:
            out, short, close, sems = rest

        def fetch(i):
            where = aligned(i * ROW_BLOCK, ROW_BLOCK)
            source = aligned(begin + i * ROW_BLOCK, ROW_BLOCK)
            return pltpu.make_async_copy(d.at[source, :], close.at[where, :], sems.at[i])

        def work(i):
            where = aligned(i * ROW_BLOCK, ROW_BLOCK)
            product = jnp.dot(close[where, :], v[...], preferred_element_type=F32)
            if moved is not None:
                product = u[where, :] - a[...] * product
            out[where, :] = product
            short[where, :] = product.astype(BF16)

        streamed(fetch, steps, work)

    args, specs = [design, vector], [ANYWHERE, NEAR]
    if moved is not None:
        args, specs = args + [moved, alpha], specs + [NEAR, NEAR]
    outs = [((rows, fits), F32), ((rows, fits), BF16)]
    scratch = [pltpu.SemaphoreType.DMA((steps,))]
    if keep:
        outs.append(((rows, width), BF16))
    else:
        scratch.insert(0, pltpu.VMEM((rows, width), BF16))
    cost = price(rows, width, fits)
    made = called(kernel, args, specs, outs, cost, scratch, False)
    return made if keep else [*made, None]


def start_back(side, design, vectors):
    rows, width = design.shape
    fits = vectors.shape[1]
    half, block = width // 2, START_BLOCK
    steps = half // block

    def kernel(s, d, v, out, turned, held, sems):
        def fetch(i):
            return pltpu.make_async_copy(
                d.at[:, aligned(s[0] * half + i * block, block)], held.at[i], sems.at[i]
            )

        turned[...] = v[...].T

        def work(i):
            product = jnp.dot(turned[...], held[i], preferred_element_type=F32)
            out[aligned(i * block, block), :] = product.T.astype(BF16)

        streamed(fetch, steps, work)

    return called(
        kernel,
        [side, design, vectors],
        [SCALAR, ANYWHERE, NEAR],
        [((half, fits), BF16)],
        price(rows, half, fits),
        [
            pltpu.VMEM((fits, rows), BF16),
            pltpu.VMEM((steps, rows, block), BF16),
            pltpu.SemaphoreType.DMA((steps,)),
        ],
        False,
    )[0]


def joined(own, other, prior, ratio):
    total = own[...].astype(F32) + other[...].astype(F32)
    if prior is not None:
        total = total + ratio[...] * prior[...]
    return total


def back_first(design, own, other, prior, ratio):
    rows, width = own.shape[0], design.shape[1]
    fits = own.shape[1]
    follow = prior is not None

    def kernel(d, own_ref, other_ref, *rest):
        prior_ref = ratio_ref = None
        if follow:
            prior_ref, ratio_ref, *rest = rest
        out, image, norm, turned = rest
        total = joined(own_ref, other_ref, prior_ref, ratio_ref)
        image[...] = total
        norm[...] = jnp.sum(total * total, axis=0, keepdims=True)
        turned[...] = total.astype(BF16).T

        @pl.loop(0, width // COL_BLOCK)
        def _(i):
            where = aligned(i * COL_BLOCK, COL_BLOCK)
            block = d[:, where]
            product = jnp.dot(turned[...], block, preferred_element_type=F32)
            out[where, :] = product.T

    args, specs = [design, own, other], [NEAR, NEAR, NEAR]
    if follow:
        args, specs = args + [prior, ratio], specs + [NEAR, NEAR]
    return called(
        kernel,
        args,
        specs,
        [((width, fits), F32), ((rows, fits), F32), ((1, fits), F32)],
        price(rows, width, fits),
        [pltpu.VMEM((fits, rows), BF16)],
    )


def back_given(side, design, own, other, prior, ratio, begun, norm_first):
    rows, width = own.shape[0], design.shape[1]
    fits = own.shape[1]
    half = width // 2
    follow = prior is not None

    def kernel(s, d, own_ref, other_ref, begun_ref, norm_ref, *rest):
        prior_ref = ratio_ref = None
        if follow:
            prior_ref, ratio_ref, *rest = rest
        out, image, turned, norm = rest
        total = joined(own_ref, other_ref, prior_ref, ratio_ref)
        image[...] = total
        turned[...] = total.astype(BF16).T
        norms = norm_ref[...] + jnp.sum(total * total, axis=0, keepdims=True)
        norm[...] = norms
        high = norms.astype(BF16).astype(F32)
        middle = (norms - high).astype(BF16).astype(F32)
        low = norms - high - middle
        row = lax.broadcasted_iota(jnp.int32, (EXTRA, fits), 0)
        below = jnp.where(row == 0, high, jnp.where(row == 1, middle, low))
        out[pl.ds(half, EXTRA), :] = jnp.where(row < 3, below, 0.0).astype(BF16)

        @pl.loop(0, half // COL_BLOCK)
        def _(i):
            where = aligned(s[0] * half + i * COL_BLOCK, COL_BLOCK)
            block = d[:, where]
            product = jnp.dot(turned[...], block, preferred_element_type=F32).T
            product = product + begun_ref[where, :]
            out[aligned(i * COL_BLOCK, COL_BLOCK), :] = product.astype(BF16)

    args = [side, design, own, other, begun, norm_first]
    specs = [SCALAR, NEAR, NEAR, NEAR, NEAR, NEAR]
    if follow:
        args, specs = args + [prior, ratio], specs + [NEAR, NEAR]
    return called(
        kernel,
        args,
        specs,
        [
            ((half + EXTRA, fits), BF16),
            ((rows, fits), F32),
            ((fits, rows), BF16),
            ((1, fits), F32),
        ],
        price(rows, half, fits),
    )


def back_kept(side, design, turned, begun):
    fits, rows = turned.shape
    half = design.shape[1] // 2

    def kernel(s, d, t, begun_ref, out):
        @pl.loop(0, half // COL_BLOCK)
        def _(i):
            where = aligned(s[0] * half + i * COL_BLOCK, COL_BLOCK)
            block = d[:, where]
            product = jnp.dot(t[...], block, preferred_element_type=F32).T
            out[aligned(i * COL_BLOCK, COL_BLOCK), :] = product + begun_ref[where, :]

    return called(
        kernel,
        [side, design, turned, begun],
        [SCALAR, NEAR, NEAR, NEAR],
        [((half, fits), F32)],
        price(rows, half, fits),
    )[0]


def exchanged(pieces):
    return lax.all_to_all(pieces, CHIPS, split_axis=0, concat_axis=0, tiled=True)


def whole_half(share, square):
    core = lax.axis_index(CORE)
    chips = lax.axis_size(CHIPS)
    rows, fits = share.shape
    scaled = (share * square).astype(BF16)
    half = exchanged(jnp.broadcast_to(scaled, (chips, rows, fits))).reshape(-1, fits)
    other = swapped(half, CORE)
    low = jnp.where(core == 0, half, other)
    high = jnp.where(core == 0, other, half)
    return jnp.concatenate([low, high], axis=0)


def per_device(design, targets, col_scale):
    core = lax.axis_index(CORE)
    chips = lax.axis_size(CHIPS)
    width, fits = design.shape[1], targets.shape[1]
    total = targets.shape[0]
    depth = total * 5 // 8
    half = width // 2
    mine = core.astype(jnp.int32).reshape(1)
    theirs = 1 - mine
    rows = half // chips
    own = core * chips + lax.axis_index(CHIPS)
    square = lax.dynamic_slice_in_dim(col_scale, own * rows, rows, 0)[:, None]
    square = square * square
    weight = 1.0 / (col_scale * col_scale)[:, None]
    count = fits // lax.axis_size(ROWS)
    first = lax.axis_index(ROWS) * count
    picks = lax.broadcasted_iota(jnp.int32, (count, fits), 1)
    picks = picks == first + lax.broadcasted_iota(jnp.int32, (count, fits), 0)
    picks = picks.astype(BF16)

    def picked(vector):
        return lax.dot_general(
            picks, vector, (((1,), (1,)), ((), ())), preferred_element_type=F32
        )

    def picked_row(values):
        return lax.dynamic_slice_in_dim(values, first, count, 1).reshape(count, 1)

    def weighed(values):
        return jnp.sum(values * values * weight, axis=0, keepdims=True)

    given = start_back(theirs, design, targets)
    arrived = swapped(given, CORE)
    kept = start_back(mine, design, targets)
    both = (kept.astype(F32) + arrived.astype(F32)).astype(BF16)
    both, square, weight = lax.optimization_barrier((both, square, weight))
    share = exchanged(both.reshape(chips, rows, fits)).astype(F32).sum(axis=0)
    back = whole_half(share, square)
    gradient = None
    narrow = picked(back)
    narrow_dir = narrow
    narrow_fit = jnp.zeros_like(narrow)
    residual = [targets[:depth].astype(F32), targets[depth:].astype(F32)]
    alpha = ratio = gamma = None
    moved, image = [None, None], [None, None]
    for step in range(ITERS):
        keep = step + 1 < ITERS
        moved_first, short_first, rows_first = image_step(
            design, back, 0, depth, keep, moved[0], alpha
        )
        other_first = swapped(short_first, COLS)
        short_first, back = lax.optimization_barrier((short_first, back))
        if step:
            gradient = gradient - alpha * back.astype(F32)
        else:
            gradient = back.astype(F32)
        part = weighed(gradient)
        part, back, gradient = lax.optimization_barrier((part, back, gradient))
        gamma_new = part + swapped(part, COLS)
        moved_second, short_second, rows_second = image_step(
            design, back, depth, total - depth, keep, moved[1], alpha
        )
        other_second = swapped(short_second, COLS)
        moved = [moved_first, moved_second]
        if step:
            image, back, short_second = lax.optimization_barrier(
                (image, back, short_second)
            )
            residual = [r - alpha * q for r, q in zip(residual, image)]
            narrow_alpha = picked_row(alpha)
            narrow_fit = narrow_fit + narrow_alpha * narrow_dir
            narrow = narrow - narrow_alpha * picked(back)
            ratio = gamma_new / gamma
            narrow_dir = narrow + picked_row(ratio) * narrow_dir
            (residual, narrow, narrow_fit, narrow_dir, gradient, other_second) = (
                lax.optimization_barrier(
                    (residual, narrow, narrow_fit, narrow_dir, gradient, other_second)
                )
            )
        gamma = gamma_new
        if step + 1 < ITERS:
            begun, image_first, norm = back_first(
                rows_first, short_first, other_first, image[0], ratio
            )
            given, image_second, turned, norm = back_given(
                theirs, rows_second, short_second, other_second, image[1], ratio, begun, norm
            )
            arrived = swapped(given, CORE)
            kept = back_kept(mine, rows_second, turned, begun)
            image = [image_first, image_second]
            both = (kept + arrived[:half].astype(F32)).astype(BF16)
            norms = norm + jnp.sum(arrived[half:].astype(F32), axis=0, keepdims=True)
            high = lax.reduce_precision(norms, 8, 7)
            middle = lax.reduce_precision(norms - high, 8, 7)
            low = norms - high - middle
            below = jnp.concatenate([high, middle, low], axis=0).astype(BF16)
            below = jnp.pad(below, ((0, EXTRA - 3), (0, 0)))
            pieces = jnp.concatenate(
                [both.reshape(chips, rows, fits), jnp.broadcast_to(below, (chips, EXTRA, fits))],
                axis=1,
            )
            sums = exchanged(pieces).astype(F32).sum(axis=0)
            delta = jnp.sum(sums[rows:], axis=0, keepdims=True)
            alpha = gamma / delta
            back = whole_half(sums[:rows], square)
        else:
            pairs = zip((short_first, short_second), (other_first, other_second), image)
            image = [a.astype(F32) + b.astype(F32) + ratio * q for a, b, q in pairs]
            norm = sum(jnp.sum(q * q, axis=0) for q in image)
            copies = jnp.broadcast_to(norm, (lax.axis_size(ROWS), 1, fits))
            copies = lax.all_to_all(copies, ROWS, split_axis=0, concat_axis=0, tiled=True)
            delta = copies.sum(axis=0)
            alpha = gamma / delta
    residual = [r - alpha * q for r, q in zip(residual, image)]
    narrow_fit = narrow_fit + picked_row(alpha) * narrow_dir
    part = (narrow_fit / col_scale).T
    return part, jnp.concatenate(residual, axis=0)


def solution(mesh):
    split = Mesh(
        mesh.devices.reshape(2, 4, 4, 2, mesh.shape["cols"]),
        ("rows_0", "rows_1", "rows_2", "rows_3", "cols"),
    )
    in_specs = (P(ROWS, "cols"), P(ROWS, None), P("cols"))
    out_specs = (P("cols", ROWS), P(ROWS, None))
    return jax.shard_map(
        per_device, mesh=split, in_specs=in_specs, out_specs=out_specs, check_vma=False
    )
```

```python
import jax
import jax.numpy as jnp
from jax import lax
from jax.experimental import pallas as pl
from jax.experimental.pallas import tpu as pltpu
from jax.sharding import Mesh
from jax.sharding import PartitionSpec as P

ITERS = 6
CHIPS = ("rows_0", "rows_1", "rows_2")
CORE = "rows_3"
ROWS = ("rows_0", "rows_1", "rows_2", "rows_3")
COLS = "cols"
BF16 = jnp.bfloat16
F32 = jnp.float32
EXTRA = 8
COL_BLOCK = 768
START_BLOCK = 256
FAR_VMEM = 42 * 1024 * 1024
NEAR_VMEM = 8 * 1024 * 1024


def swapped(array, axis):
    return lax.ppermute(array, axis, ((0, 1), (1, 0)))


def settings(near):
    return pltpu.CompilerParams(vmem_limit_bytes=NEAR_VMEM if near else FAR_VMEM)


def price(rows, cols, fits):
    return pl.CostEstimate(
        flops=2 * rows * cols * fits, bytes_accessed=2 * rows * cols, transcendentals=0
    )


ANYWHERE = pl.BlockSpec(memory_space=pltpu.HBM)
NEAR = pl.BlockSpec(memory_space=pltpu.VMEM)
SCALAR = pl.BlockSpec(memory_space=pltpu.SMEM)


def called(kernel, ins, specs, outs, cost, scratch=(), near=True):
    return pl.pallas_call(
        kernel,
        in_specs=specs,
        out_specs=[NEAR] * len(outs),
        out_shape=[jax.ShapeDtypeStruct(shape, dtype) for shape, dtype in outs],
        scratch_shapes=list(scratch),
        compiler_params=settings(near),
        cost_estimate=cost,
    )(*ins)


def streamed(fetch, steps, work):
    @pl.loop(0, steps)
    def _(i):
        fetch(i).start()

    def ready(i):
        fetch(i).wait()
        work(i)

    pl.loop(0, steps)(ready)


def aligned(start, size):
    return pl.ds(pl.multiple_of(start, size), size)


def image_step(design, vector, begin, rows, moved=None, alpha=None):
    block = lax.slice_in_dim(design, begin, begin + rows, axis=0)
    product = jnp.dot(block, vector, preferred_element_type=F32)
    product = lax.optimization_barrier(product)
    if moved is not None:
        product = moved - alpha * product
    return product, product.astype(BF16)


def start_back(side, design, vectors):
    rows, width = design.shape
    fits = vectors.shape[1]
    half, block = width // 2, START_BLOCK
    steps = half // block

    def kernel(s, d, v, out, turned, held, sems):
        def fetch(i):
            return pltpu.make_async_copy(
                d.at[:, aligned(s[0] * half + i * block, block)], held.at[i], sems.at[i]
            )

        turned[...] = v[...].T

        def work(i):
            product = jnp.dot(turned[...], held[i], preferred_element_type=F32)
            out[aligned(i * block, block), :] = product.T.astype(BF16)

        streamed(fetch, steps, work)

    return called(
        kernel,
        [side, design, vectors],
        [SCALAR, ANYWHERE, NEAR],
        [((half, fits), BF16)],
        price(rows, half, fits),
        [
            pltpu.VMEM((fits, rows), BF16),
            pltpu.VMEM((steps, rows, block), BF16),
            pltpu.SemaphoreType.DMA((steps,)),
        ],
        False,
    )[0]


def joined(own, other, prior, ratio):
    total = own[...].astype(F32) + other[...].astype(F32)
    if prior is not None:
        total = total + ratio[...] * prior[...]
    return total


def back_first(design, own, other, prior, ratio):
    rows, fits = own.shape
    total_rows, width = design.shape
    steps = width // COL_BLOCK
    follow = prior is not None

    def kernel(d, own_ref, other_ref, *rest):
        prior_ref = ratio_ref = None
        if follow:
            prior_ref, ratio_ref, *rest = rest
        out, image, norm, close, turned, held, sems, last = rest

        def fetch(i):
            where = aligned(i * COL_BLOCK, COL_BLOCK)
            return pltpu.make_async_copy(d.at[pl.ds(0, rows), where], held.at[i], sems.at[i])

        @pl.loop(0, steps)
        def _(i):
            fetch(i).start()

        later = pltpu.make_async_copy(d.at[pl.ds(rows, total_rows - rows), :], close, last)
        later.start()
        total = joined(own_ref, other_ref, prior_ref, ratio_ref)
        image[...] = total
        norm[...] = jnp.sum(total * total, axis=0, keepdims=True)
        turned[...] = total.astype(BF16).T

        @pl.loop(0, steps)
        def _(i):
            fetch(i).wait()
            where = aligned(i * COL_BLOCK, COL_BLOCK)
            product = jnp.dot(turned[...], held[i], preferred_element_type=F32)
            out[where, :] = product.T

        later.wait()

    args, specs = [design, own, other], [ANYWHERE, NEAR, NEAR]
    if follow:
        args, specs = args + [prior, ratio], specs + [NEAR, NEAR]
    return called(
        kernel,
        args,
        specs,
        [
            ((width, fits), F32),
            ((rows, fits), F32),
            ((1, fits), F32),
            ((total_rows - rows, width), BF16),
        ],
        price(rows, width, fits),
        [
            pltpu.VMEM((fits, rows), BF16),
            pltpu.VMEM((steps, rows, COL_BLOCK), BF16),
            pltpu.SemaphoreType.DMA((steps,)),
            pltpu.SemaphoreType.DMA,
        ],
        False,
    )


def back_given(side, design, own, other, prior, ratio, begun, norm_first):
    rows, width = own.shape[0], design.shape[1]
    fits = own.shape[1]
    half = width // 2
    follow = prior is not None

    def kernel(s, d, own_ref, other_ref, begun_ref, norm_ref, *rest):
        prior_ref = ratio_ref = None
        if follow:
            prior_ref, ratio_ref, *rest = rest
        out, image, turned, norm = rest
        total = joined(own_ref, other_ref, prior_ref, ratio_ref)
        image[...] = total
        turned[...] = total.astype(BF16).T
        norms = norm_ref[...] + jnp.sum(total * total, axis=0, keepdims=True)
        norm[...] = norms
        high = norms.astype(BF16).astype(F32)
        middle = (norms - high).astype(BF16).astype(F32)
        low = norms - high - middle
        row = lax.broadcasted_iota(jnp.int32, (EXTRA, fits), 0)
        below = jnp.where(row == 0, high, jnp.where(row == 1, middle, low))
        out[pl.ds(half, EXTRA), :] = jnp.where(row < 3, below, 0.0).astype(BF16)

        @pl.loop(0, half // COL_BLOCK)
        def _(i):
            where = aligned(s[0] * half + i * COL_BLOCK, COL_BLOCK)
            block = d[:, where]
            product = jnp.dot(turned[...], block, preferred_element_type=F32).T
            product = product + begun_ref[where, :]
            out[aligned(i * COL_BLOCK, COL_BLOCK), :] = product.astype(BF16)

    args = [side, design, own, other, begun, norm_first]
    specs = [SCALAR, NEAR, NEAR, NEAR, NEAR, NEAR]
    if follow:
        args, specs = args + [prior, ratio], specs + [NEAR, NEAR]
    return called(
        kernel,
        args,
        specs,
        [
            ((half + EXTRA, fits), BF16),
            ((rows, fits), F32),
            ((fits, rows), BF16),
            ((1, fits), F32),
        ],
        price(rows, half, fits),
    )


def back_kept(side, design, turned, begun):
    fits, rows = turned.shape
    half = design.shape[1] // 2

    def kernel(s, d, t, begun_ref, out):
        @pl.loop(0, half // COL_BLOCK)
        def _(i):
            where = aligned(s[0] * half + i * COL_BLOCK, COL_BLOCK)
            block = d[:, where]
            product = jnp.dot(t[...], block, preferred_element_type=F32).T
            out[aligned(i * COL_BLOCK, COL_BLOCK), :] = product + begun_ref[where, :]

    return called(
        kernel,
        [side, design, turned, begun],
        [SCALAR, NEAR, NEAR, NEAR],
        [((half, fits), F32)],
        price(rows, half, fits),
    )[0]


def exchanged(pieces):
    return lax.all_to_all(pieces, CHIPS, split_axis=0, concat_axis=0, tiled=True)


def whole_half(share, square):
    core = lax.axis_index(CORE)
    chips = lax.axis_size(CHIPS)
    rows, fits = share.shape
    scaled = (share * square).astype(BF16)
    half = exchanged(jnp.broadcast_to(scaled, (chips, rows, fits))).reshape(-1, fits)
    other = swapped(half, CORE)
    low = jnp.where(core == 0, half, other)
    high = jnp.where(core == 0, other, half)
    return lax.optimization_barrier(jnp.concatenate([low, high], axis=0))


def per_device(design, targets, col_scale):
    core = lax.axis_index(CORE)
    chips = lax.axis_size(CHIPS)
    width, fits = design.shape[1], targets.shape[1]
    total = targets.shape[0]
    depth = total // 2
    half = width // 2
    mine = core.astype(jnp.int32).reshape(1)
    theirs = 1 - mine
    rows = half // chips
    own = core * chips + lax.axis_index(CHIPS)
    square = lax.dynamic_slice_in_dim(col_scale, own * rows, rows, 0)[:, None]
    square = square * square
    weight = 1.0 / (col_scale * col_scale)[:, None]
    count = fits // lax.axis_size(ROWS)
    first = lax.axis_index(ROWS) * count
    picks = lax.broadcasted_iota(jnp.int32, (count, fits), 1)
    picks = picks == first + lax.broadcasted_iota(jnp.int32, (count, fits), 0)
    picks = picks.astype(BF16)

    def picked(vector):
        return lax.dot_general(
            picks, vector, (((1,), (1,)), ((), ())), preferred_element_type=F32
        )

    def picked_row(values):
        return lax.dynamic_slice_in_dim(values, first, count, 1).reshape(count, 1)

    def weighed(values):
        return jnp.sum(values * values * weight, axis=0, keepdims=True)

    given = start_back(theirs, design, targets)
    arrived = swapped(given, CORE)
    kept = start_back(mine, design, targets)
    both = (kept.astype(F32) + arrived.astype(F32)).astype(BF16)
    both, square, weight = lax.optimization_barrier((both, square, weight))
    share = exchanged(both.reshape(chips, rows, fits)).astype(F32).sum(axis=0)
    back = whole_half(share, square)
    gradient = None
    narrow = picked(back)
    narrow_dir = narrow
    narrow_fit = jnp.zeros_like(narrow)
    residual = [targets[:depth].astype(F32), targets[depth:].astype(F32)]
    alpha = ratio = gamma = None
    moved, image = [None, None], [None, None]
    for step in range(ITERS):
        moved_first, short_first = image_step(
            design, back, 0, depth, moved[0], alpha
        )
        other_first = swapped(short_first, COLS)
        short_first, back = lax.optimization_barrier((short_first, back))
        if step:
            gradient = gradient - alpha * back.astype(F32)
        else:
            gradient = back.astype(F32)
        part = weighed(gradient)
        part, back, gradient = lax.optimization_barrier((part, back, gradient))
        gamma_new = part + swapped(part, COLS)
        moved_second, short_second = image_step(design, back, depth, total - depth, moved[1], alpha)
        other_second = swapped(short_second, COLS)
        moved = [moved_first, moved_second]
        if step:
            image, back, short_second = lax.optimization_barrier(
                (image, back, short_second)
            )
            residual = [r - alpha * q for r, q in zip(residual, image)]
            narrow_alpha = picked_row(alpha)
            narrow_fit = narrow_fit + narrow_alpha * narrow_dir
            narrow = narrow - narrow_alpha * picked(back)
            ratio = gamma_new / gamma
            narrow_dir = narrow + picked_row(ratio) * narrow_dir
            (residual, narrow, narrow_fit, narrow_dir, gradient, other_second) = (
                lax.optimization_barrier(
                    (residual, narrow, narrow_fit, narrow_dir, gradient, other_second)
                )
            )
        gamma = gamma_new
        if step + 1 < ITERS:
            begun, image_first, norm, rows_second = back_first(
                design, short_first, other_first, image[0], ratio
            )
            given, image_second, turned, norm = back_given(
                theirs, rows_second, short_second, other_second, image[1], ratio, begun, norm
            )
            arrived = swapped(given, CORE)
            kept = back_kept(mine, rows_second, turned, begun)
            image = [image_first, image_second]
            both = (kept + arrived[:half].astype(F32)).astype(BF16)
            norms = norm + jnp.sum(arrived[half:].astype(F32), axis=0, keepdims=True)
            high = lax.reduce_precision(norms, 8, 7)
            middle = lax.reduce_precision(norms - high, 8, 7)
            low = norms - high - middle
            below = jnp.concatenate([high, middle, low], axis=0).astype(BF16)
            below = jnp.pad(below, ((0, EXTRA - 3), (0, 0)))
            pieces = jnp.concatenate(
                [both.reshape(chips, rows, fits), jnp.broadcast_to(below, (chips, EXTRA, fits))],
                axis=1,
            )
            sums = exchanged(pieces).astype(F32).sum(axis=0)
            delta = jnp.sum(sums[rows:], axis=0, keepdims=True)
            alpha = gamma / delta
            back = whole_half(sums[:rows], square)
        else:
            pairs = zip((short_first, short_second), (other_first, other_second), image)
            image = [a.astype(F32) + b.astype(F32) + ratio * q for a, b, q in pairs]
            norm = sum(jnp.sum(q * q, axis=0) for q in image)
            copies = jnp.broadcast_to(norm, (lax.axis_size(ROWS), 1, fits))
            copies = lax.all_to_all(copies, ROWS, split_axis=0, concat_axis=0, tiled=True)
            delta = copies.sum(axis=0)
            alpha = gamma / delta
    residual = [r - alpha * q for r, q in zip(residual, image)]
    narrow_fit = narrow_fit + picked_row(alpha) * narrow_dir
    part = (narrow_fit / col_scale).T
    return part, jnp.concatenate(residual, axis=0)


def solution(mesh):
    split = Mesh(
        mesh.devices.reshape(2, 4, 4, 2, mesh.shape["cols"]),
        ("rows_0", "rows_1", "rows_2", "rows_3", "cols"),
    )
    in_specs = (P(ROWS, "cols"), P(ROWS, None), P("cols"))
    out_specs = (P("cols", ROWS), P(ROWS, None))
    return jax.shard_map(
        per_device, mesh=split, in_specs=in_specs, out_specs=out_specs, check_vma=False
    )
```

```python
import jax
import jax.numpy as jnp
from jax import lax
from jax.experimental import pallas as pl
from jax.experimental.pallas import tpu as pltpu
from jax.sharding import Mesh
from jax.sharding import PartitionSpec as P

ITERS = 6
CHIPS = ("rows_0", "rows_1", "rows_2")
CORE = "rows_3"
ROWS = ("rows_0", "rows_1", "rows_2", "rows_3")
COLS = "cols"
BF16 = jnp.bfloat16
F32 = jnp.float32
EXTRA = 8
ROW_BLOCK = 128
COL_BLOCK = 512
START_BLOCK = 256
FAR_VMEM = 42 * 1024 * 1024
NEAR_VMEM = 8 * 1024 * 1024


def swapped(array, axis):
    return lax.ppermute(array, axis, ((0, 1), (1, 0)))


def settings(near):
    return pltpu.CompilerParams(vmem_limit_bytes=NEAR_VMEM if near else FAR_VMEM)


def price(rows, cols, fits):
    return pl.CostEstimate(
        flops=2 * rows * cols * fits, bytes_accessed=2 * rows * cols, transcendentals=0
    )


ANYWHERE = pl.BlockSpec(memory_space=pltpu.HBM)
NEAR = pl.BlockSpec(memory_space=pltpu.VMEM)
SCALAR = pl.BlockSpec(memory_space=pltpu.SMEM)


def called(kernel, ins, specs, outs, cost, scratch=(), near=True):
    return pl.pallas_call(
        kernel,
        in_specs=specs,
        out_specs=[NEAR] * len(outs),
        out_shape=[jax.ShapeDtypeStruct(shape, dtype) for shape, dtype in outs],
        scratch_shapes=list(scratch),
        compiler_params=settings(near),
        cost_estimate=cost,
    )(*ins)


def streamed(fetch, steps, work):
    @pl.loop(0, steps)
    def _(i):
        fetch(i).start()

    def ready(i):
        fetch(i).wait()
        work(i)

    pl.loop(0, steps)(ready)


def aligned(start, size):
    return pl.ds(pl.multiple_of(start, size), size)


def image_step(design, vector, begin, rows, keep, moved=None, alpha=None):
    width, fits = design.shape[1], vector.shape[1]
    block = ROW_BLOCK if begin or not keep else 2 * ROW_BLOCK
    steps = rows // block

    def kernel(d, v, *rest):
        if moved is not None:
            u, a, out, short, close, sems = rest
        else:
            out, short, close, sems = rest

        def fetch(i):
            where = aligned(i * block, block)
            source = aligned(begin + i * block, block)
            return pltpu.make_async_copy(d.at[source, :], close.at[where, :], sems.at[i])

        def work(i):
            where = aligned(i * block, block)
            product = jnp.dot(close[where, :], v[...], preferred_element_type=F32)
            if moved is not None:
                product = u[where, :] - a[...] * product
            out[where, :] = product
            short[where, :] = product.astype(BF16)

        streamed(fetch, steps, work)

    args, specs = [design, vector], [ANYWHERE, NEAR]
    if moved is not None:
        args, specs = args + [moved, alpha], specs + [NEAR, NEAR]
    outs = [((rows, fits), F32), ((rows, fits), BF16)]
    scratch = [pltpu.SemaphoreType.DMA((steps,))]
    if keep:
        outs.append(((rows, width), BF16))
    else:
        scratch.insert(0, pltpu.VMEM((rows, width), BF16))
    cost = price(rows, width, fits)
    made = called(kernel, args, specs, outs, cost, scratch, False)
    return made if keep else [*made, None]


def start_back(side, design, vectors):
    rows, width = design.shape
    fits = vectors.shape[1]
    half, block = width // 2, START_BLOCK
    steps = half // block

    def kernel(s, d, v, out, turned, held, sems):
        def fetch(i):
            return pltpu.make_async_copy(
                d.at[:, aligned(s[0] * half + i * block, block)], held.at[i], sems.at[i]
            )

        turned[...] = v[...].T

        def work(i):
            product = jnp.dot(turned[...], held[i], preferred_element_type=F32)
            out[aligned(i * block, block), :] = product.T.astype(BF16)

        streamed(fetch, steps, work)

    return called(
        kernel,
        [side, design, vectors],
        [SCALAR, ANYWHERE, NEAR],
        [((half, fits), BF16)],
        price(rows, half, fits),
        [
            pltpu.VMEM((fits, rows), BF16),
            pltpu.VMEM((steps, rows, block), BF16),
            pltpu.SemaphoreType.DMA((steps,)),
        ],
        False,
    )[0]


def joined(own, other, prior, ratio):
    total = own[...].astype(F32) + other[...].astype(F32)
    if prior is not None:
        total = total + ratio[...] * prior[...]
    return total


def back_first(design, own, other, prior, ratio):
    rows, width = own.shape[0], design.shape[1]
    fits = own.shape[1]
    follow = prior is not None

    def kernel(d, own_ref, other_ref, *rest):
        prior_ref = ratio_ref = None
        if follow:
            prior_ref, ratio_ref, *rest = rest
        out, image, norm, turned = rest
        total = joined(own_ref, other_ref, prior_ref, ratio_ref)
        image[...] = total
        norm[...] = jnp.sum(total * total, axis=0, keepdims=True)
        turned[...] = total.astype(BF16).T

        @pl.loop(0, width // COL_BLOCK)
        def _(i):
            where = aligned(i * COL_BLOCK, COL_BLOCK)
            block = d[:, where]
            product = jnp.dot(turned[...], block, preferred_element_type=F32)
            out[where, :] = product.T

    args, specs = [design, own, other], [NEAR, NEAR, NEAR]
    if follow:
        args, specs = args + [prior, ratio], specs + [NEAR, NEAR]
    return called(
        kernel,
        args,
        specs,
        [((width, fits), F32), ((rows, fits), F32), ((1, fits), F32)],
        price(rows, width, fits),
        [pltpu.VMEM((fits, rows), BF16)],
    )


def back_given(side, design, own, other, prior, ratio, begun, norm_first):
    rows, width = own.shape[0], design.shape[1]
    fits = own.shape[1]
    half = width // 2
    follow = prior is not None

    def kernel(s, d, own_ref, other_ref, begun_ref, norm_ref, *rest):
        prior_ref = ratio_ref = None
        if follow:
            prior_ref, ratio_ref, *rest = rest
        out, image, turned, norm = rest
        total = joined(own_ref, other_ref, prior_ref, ratio_ref)
        image[...] = total
        turned[...] = total.astype(BF16).T
        norms = norm_ref[...] + jnp.sum(total * total, axis=0, keepdims=True)
        norm[...] = norms
        high = norms.astype(BF16).astype(F32)
        middle = (norms - high).astype(BF16).astype(F32)
        low = norms - high - middle
        row = lax.broadcasted_iota(jnp.int32, (EXTRA, fits), 0)
        below = jnp.where(row == 0, high, jnp.where(row == 1, middle, low))
        out[pl.ds(half, EXTRA), :] = jnp.where(row < 3, below, 0.0).astype(BF16)

        @pl.loop(0, half // COL_BLOCK)
        def _(i):
            where = aligned(s[0] * half + i * COL_BLOCK, COL_BLOCK)
            block = d[:, where]
            product = jnp.dot(turned[...], block, preferred_element_type=F32).T
            product = product + begun_ref[where, :]
            out[aligned(i * COL_BLOCK, COL_BLOCK), :] = product.astype(BF16)

    args = [side, design, own, other, begun, norm_first]
    specs = [SCALAR, NEAR, NEAR, NEAR, NEAR, NEAR]
    if follow:
        args, specs = args + [prior, ratio], specs + [NEAR, NEAR]
    return called(
        kernel,
        args,
        specs,
        [
            ((half + EXTRA, fits), BF16),
            ((rows, fits), F32),
            ((fits, rows), BF16),
            ((1, fits), F32),
        ],
        price(rows, half, fits),
    )


def back_kept(side, design, turned, begun):
    fits, rows = turned.shape
    half = design.shape[1] // 2

    def kernel(s, d, t, begun_ref, out):
        @pl.loop(0, half // COL_BLOCK)
        def _(i):
            where = aligned(s[0] * half + i * COL_BLOCK, COL_BLOCK)
            block = d[:, where]
            product = jnp.dot(t[...], block, preferred_element_type=F32).T
            out[aligned(i * COL_BLOCK, COL_BLOCK), :] = product + begun_ref[where, :]

    return called(
        kernel,
        [side, design, turned, begun],
        [SCALAR, NEAR, NEAR, NEAR],
        [((half, fits), F32)],
        price(rows, half, fits),
    )[0]


def exchanged(pieces):
    return lax.all_to_all(pieces, CHIPS, split_axis=0, concat_axis=0, tiled=True)


def whole_half(share, square):
    core = lax.axis_index(CORE)
    chips = lax.axis_size(CHIPS)
    rows, fits = share.shape
    scaled = (share * square).astype(BF16)
    half = exchanged(jnp.broadcast_to(scaled, (chips, rows, fits))).reshape(-1, fits)
    other = swapped(half, CORE)
    low = jnp.where(core == 0, half, other)
    high = jnp.where(core == 0, other, half)
    return jnp.concatenate([low, high], axis=0)


def per_device(design, targets, col_scale):
    core = lax.axis_index(CORE)
    chips = lax.axis_size(CHIPS)
    width, fits = design.shape[1], targets.shape[1]
    total = targets.shape[0]
    depth = total * 5 // 8
    half = width // 2
    mine = core.astype(jnp.int32).reshape(1)
    theirs = 1 - mine
    rows = half // chips
    own = core * chips + lax.axis_index(CHIPS)
    square = lax.dynamic_slice_in_dim(col_scale, own * rows, rows, 0)[:, None]
    square = square * square
    weight = 1.0 / (col_scale * col_scale)[:, None]
    count = fits // lax.axis_size(ROWS)
    first = lax.axis_index(ROWS) * count
    picks = lax.broadcasted_iota(jnp.int32, (count, fits), 1)
    picks = picks == first + lax.broadcasted_iota(jnp.int32, (count, fits), 0)
    picks = picks.astype(BF16)

    def picked(vector):
        return lax.dot_general(
            picks, vector, (((1,), (1,)), ((), ())), preferred_element_type=F32
        )

    def picked_row(values):
        return lax.dynamic_slice_in_dim(values, first, count, 1).reshape(count, 1)

    def weighed(values):
        return jnp.sum(values * values * weight, axis=0, keepdims=True)

    given = start_back(theirs, design, targets)
    arrived = swapped(given, CORE)
    kept = start_back(mine, design, targets)
    both = (kept.astype(F32) + arrived.astype(F32)).astype(BF16)
    both, square, weight = lax.optimization_barrier((both, square, weight))
    share = exchanged(both.reshape(chips, rows, fits)).astype(F32).sum(axis=0)
    back = whole_half(share, square)
    gradient = None
    narrow = picked(back)
    narrow_dir = narrow
    narrow_fit = jnp.zeros_like(narrow)
    residual = [targets[:depth].astype(F32), targets[depth:].astype(F32)]
    alpha = ratio = gamma = None
    moved, image = [None, None], [None, None]
    for step in range(ITERS):
        keep = step + 1 < ITERS
        moved_first, short_first, rows_first = image_step(
            design, back, 0, depth, keep, moved[0], alpha
        )
        other_first = swapped(short_first, COLS)
        short_first, back = lax.optimization_barrier((short_first, back))
        if step:
            gradient = gradient - alpha * back.astype(F32)
        else:
            gradient = back.astype(F32)
        part = weighed(gradient)
        part, back, gradient = lax.optimization_barrier((part, back, gradient))
        gamma_new = part + swapped(part, COLS)
        moved_second, short_second, rows_second = image_step(
            design, back, depth, total - depth, keep, moved[1], alpha
        )
        other_second = swapped(short_second, COLS)
        moved = [moved_first, moved_second]
        if step:
            image, back, short_second = lax.optimization_barrier(
                (image, back, short_second)
            )
            residual = [r - alpha * q for r, q in zip(residual, image)]
            narrow_alpha = picked_row(alpha)
            narrow_fit = narrow_fit + narrow_alpha * narrow_dir
            narrow = narrow - narrow_alpha * picked(back)
            ratio = gamma_new / gamma
            narrow_dir = narrow + picked_row(ratio) * narrow_dir
            (residual, narrow, narrow_fit, narrow_dir, gradient, other_second) = (
                lax.optimization_barrier(
                    (residual, narrow, narrow_fit, narrow_dir, gradient, other_second)
                )
            )
        gamma = gamma_new
        if step + 1 < ITERS:
            begun, image_first, norm = back_first(
                rows_first, short_first, other_first, image[0], ratio
            )
            given, image_second, turned, norm = back_given(
                theirs, rows_second, short_second, other_second, image[1], ratio, begun, norm
            )
            arrived = swapped(given, CORE)
            kept = back_kept(mine, rows_second, turned, begun)
            image = [image_first, image_second]
            both = (kept + arrived[:half].astype(F32)).astype(BF16)
            norms = norm + jnp.sum(arrived[half:].astype(F32), axis=0, keepdims=True)
            high = lax.reduce_precision(norms, 8, 7)
            middle = lax.reduce_precision(norms - high, 8, 7)
            low = norms - high - middle
            below = jnp.concatenate([high, middle, low], axis=0).astype(BF16)
            below = jnp.pad(below, ((0, EXTRA - 3), (0, 0)))
            pieces = jnp.concatenate(
                [both.reshape(chips, rows, fits), jnp.broadcast_to(below, (chips, EXTRA, fits))],
                axis=1,
            )
            sums = exchanged(pieces).astype(F32).sum(axis=0)
            delta = jnp.sum(sums[rows:], axis=0, keepdims=True)
            alpha = gamma / delta
            back = whole_half(sums[:rows], square)
        else:
            pairs = zip((short_first, short_second), (other_first, other_second), image)
            image = [a.astype(F32) + b.astype(F32) + ratio * q for a, b, q in pairs]
            norm = sum(jnp.sum(q * q, axis=0) for q in image)
            norm = norm + swapped(norm, CORE)
            copies = exchanged(jnp.broadcast_to(norm, (chips, 1, fits)))
            delta = copies.sum(axis=0)
            alpha = gamma / delta
    residual = [r - alpha * q for r, q in zip(residual, image)]
    narrow_fit = narrow_fit + picked_row(alpha) * narrow_dir
    part = (narrow_fit / col_scale).T
    return part, jnp.concatenate(residual, axis=0)


def solution(mesh):
    split = Mesh(
        mesh.devices.reshape(2, 4, 4, 2, mesh.shape["cols"]),
        ("rows_0", "rows_1", "rows_2", "rows_3", "cols"),
    )
    in_specs = (P(ROWS, "cols"), P(ROWS, None), P("cols"))
    out_specs = (P("cols", ROWS), P(ROWS, None))
    return jax.shard_map(
        per_device, mesh=split, in_specs=in_specs, out_specs=out_specs, check_vma=False
    )
```
